256 devices in a mesh: seq: 64 (over z_hi, y, x), rep: 4 (over z_lo, core).
Axes of the slice: x: 4, y: 4, z: 8 (z_hi: 4, z_lo: 2; z = z_hi * 2 + z_lo), core: 2. Of those that a mesh axis runs over, the one named last changes fastest.
Arguments:
- queries: bfloat16 [32768, 2048], P(('rep', 'seq')), parts along dimension 0, may hold values from -6 to 6
- keys: bfloat16 [32768, 2048], P(('rep', 'seq')), parts along dimension 0, may hold values from -6 to 6
- values: bfloat16 [32768, 2048], P(('rep', 'seq')), parts along dimension 0, may hold values from -6 to 6
- short_taps: float32 [3, 3, 2048], replicated, may hold values from -3.5 to 3.5
- decay: float32 [2048, 16], replicated, may hold values from 6.1035156e-05 to 0.1
- residue: float32 [2048, 16], replicated, may hold values from -1.5 to 1.5
- skip: float32 [2048], replicated, may hold values from -3 to 3
- w_out: bfloat16 [2048, 2048], replicated, may hold values from -0.125 to 0.125
Outputs:
- layer_out: bfloat16 [32768, 2048], P(('rep', 'seq')), parts along dimension 0
The draws below stay inside these ranges and needn't reach their ends.
There are 4 independent parts, one for each index of `rep`. The reference program is written for one: setup_inputs(seed, part) draws one part's arguments, and reference() takes and returns one part's arrays. A program takes and returns all parts, laid end to end along the dimension named above; an argument that names none is the same for every part. Nothing has to cross between parts.
All inputs are finite; a program needn't handle non-finite values.
Results may differ from the reference program's by a relative error of at most 0.014.
Values may be sent and summed in bfloat16 or wider, within the bound.
A program may use at most 64 MiB of HBM per device.

```python
import math
import jax
import jax.numpy as jnp
from jax import lax

D = 2048
MODES = 16
SEQLEN = 8192


def levels(stream_key, extent, shards, smallest, top_value):
    level = 1.0
    for axis_at, parts in shards:
        steps = jax.random.uniform(jax.random.fold_in(jax.random.fold_in(stream_key, 6), axis_at), (parts,), jnp.float32, smallest / len(shards), top_value / len(shards))
        level = level * jnp.repeat(jnp.exp(steps), extent[axis_at] // parts).reshape((-1,) + (1,) * (len(extent) - 1 - axis_at))
    return level


def normal_values(key, extent, deviation, bound, split=(), kind=jnp.bfloat16):
    values = jax.random.normal(key, extent, jnp.float32) * deviation
    if len(split) > 0:
        values = levels(key, extent, split, -0.22, 0.18) * values
    return jnp.clip(values, min=-bound, max=bound).astype(kind)


def setup_inputs(seed: int = 0, part: int = 0) -> dict:
    seeds = jax.random.split(jax.random.key(seed), 9)
    part_keys = jax.random.split(jax.random.fold_in(seeds[8], part), 9)
    return {
        "queries": normal_values(part_keys[0], (SEQLEN, D), 1.0, 6.0, ((0, 64),)),
        "keys": normal_values(part_keys[1], (SEQLEN, D), 1.0, 6.0, ((0, 64),)),
        "values": normal_values(part_keys[2], (SEQLEN, D), 1.0, 6.0, ((0, 64),)),
        "short_taps": normal_values(seeds[3], (3, 3, D), 3 ** -0.5, 3.5, (), jnp.float32),
        "decay": jnp.clip(jnp.exp(jax.random.uniform(seeds[4], (D, MODES), jnp.float32, math.log(6.103515625e-05), math.log(0.1))), 6.103515625e-05, 0.1),
        "residue": normal_values(seeds[5], (D, MODES), 0.25, 1.5, (), jnp.float32),
        "skip": normal_values(seeds[6], (D,), 0.5, 3.0, (), jnp.float32),
        "w_out": normal_values(seeds[7], (D, D), D ** -0.5, 0.125),
    }


def short_conv(tokens, taps):
    whole = tokens.astype(jnp.float32)
    width = whole.shape[1]
    result = taps[0] * whole
    first = jnp.concatenate([jnp.zeros((1, width), jnp.float32), whole[:-1]], axis=0)
    second = jnp.concatenate([jnp.zeros((2, width), jnp.float32), whole[:-2]], axis=0)
    return result + taps[1] * first + taps[2] * second

def reference(queries, keys, values, short_taps, decay, residue, skip, w_out):
    q_short = short_conv(queries, short_taps[0])
    k_short = short_conv(keys, short_taps[1])
    v_short = short_conv(values, short_taps[2])
    mixed_in = (k_short * v_short).astype(jnp.bfloat16)
    signal = mixed_in.astype(jnp.float32)
    weights = residue * jnp.sqrt(1.0 - jnp.exp(-2.0 * decay))
    length, width = signal.shape
    group = math.gcd(width, 128)
    count = width // group
    grouped = signal.reshape(length, count, group).transpose(1, 0, 2)
    rate_groups = decay.reshape(count, group, decay.shape[1])
    weight_groups = weights.reshape(count, group, decay.shape[1])

    def one_group(items):
        piece, rates, wts = items
        times = jnp.arange(length, dtype=jnp.float32)
        filt = lax.optimization_barrier(jnp.sum(jnp.exp(-times[:, None, None] * rates[None]) * wts[None], axis=2))
        total = 2 * length
        spectrum = jnp.fft.rfft(piece, total, axis=0) * jnp.fft.rfft(filt, total, axis=0)
        return jnp.fft.irfft(spectrum, total, axis=0)[:length]
    convolved = lax.map(one_group, (grouped, rate_groups, weight_groups))
    convolved = convolved.transpose(1, 0, 2).reshape(length, width)
    long_out = (convolved + skip * signal).astype(jnp.bfloat16)
    gated = (q_short * long_out.astype(jnp.float32)).astype(jnp.bfloat16)
    return jnp.dot(gated, w_out, preferred_element_type=jnp.float32).astype(jnp.bfloat16)
```

```python
import functools

import jax
import jax.numpy as jnp
from jax import lax
from jax.experimental import pallas as pl
from jax.experimental.pallas import tpu as pltpu
from jax.sharding import PartitionSpec as P

MESH = pl.DeviceIdType.MESH
LANES = 128
ROWS = 8


def lanes(strip, count=1):
    return pl.ds(pl.multiple_of(strip * LANES, LANES), count * LANES)


def kernel(
    planes, q_hbm, k_hbm, v_hbm, taps_hbm, rate_hbm, res_hbm, skip_hbm, w_hbm, out_ref,
    q_in, k_in, v_in, tails, halos, taps, rate, res, skip, w_in,
    qf, kf, vf, x, y, gain, ends, got, sums, carry, sums_in, starts, starts_in, held, spread, gated,
    load_sem, halo_send, halo_recv, up_send, up_recv, side_send, side_recv, down_send, down_recv,
):
    toks, width = q_hbm.shape
    modes = rate_hbm.shape[0]
    strips = width // LANES
    blocks = toks // ROWS
    members = strips
    wide = min(4, strips)
    me = lax.axis_index("seq")
    plane, spot = me // members, me % members
    last = planes * members - 1

    def load(source, target, at):
        copy = pltpu.make_async_copy(source, target, load_sem.at[at])
        copy.start()
        return copy

    end_rows = pl.ds(toks - ROWS, ROWS)
    tail_loads = [load(ref.at[end_rows, :], tails.at[i], i) for i, ref in enumerate((k_hbm, v_hbm, q_hbm))]
    k_load = load(k_hbm, k_in, 3)
    v_load = load(v_hbm, v_in, 4)
    rate_load = load(rate_hbm, rate, 5)
    taps_load = load(taps_hbm, taps, 6)
    res_load = load(res_hbm, res, 7)
    skip_load = load(skip_hbm, skip, 8)
    q_load = load(q_hbm, q_in, 9)
    w_load = load(w_hbm, w_in, 10)

    barrier = pltpu.get_barrier_semaphore()

    def greet(device):
        pl.semaphore_signal(barrier, inc=1, device_id={"seq": device}, device_id_type=MESH)

    for i in range(members):

        @pl.when(spot != i)
        def _():
            greet(plane * members + i)

    for i in range(planes):

        @pl.when(plane != i)
        def _():
            greet(i * members + spot)

    first_of_plane = (spot == 0) & (plane > 0)
    last_of_plane = (spot == members - 1) & (plane < planes - 1)

    @pl.when(first_of_plane)
    def _():
        greet(me - 1)

    @pl.when(last_of_plane)
    def _():
        greet(me + 1)

    for copy in (k_load, v_load, rate_load, taps_load):
        copy.wait()

    def short(source, kind, start, count, cols):
        rows = [source[pl.ds(ROWS + start - lag, count), cols] for lag in range(3)]
        total = taps[kind, 0:1, cols] * rows[0] + taps[kind, 1:2, cols] * rows[1]
        return total + taps[kind, 2:3, cols] * rows[2]

    def mixed(start, count, cols):
        product = short(kf, 1, start, count, cols) * short(vf, 2, start, count, cols)
        x[pl.ds(start, count), cols] = product.astype(jnp.bfloat16).astype(jnp.float32)

    def first_pass(at, _):
        cols = lanes(at * wide, wide)
        kf[0:ROWS, cols] = jnp.zeros((ROWS, wide * LANES), jnp.float32)
        vf[0:ROWS, cols] = jnp.zeros((ROWS, wide * LANES), jnp.float32)
        kf[pl.ds(ROWS, toks), cols] = k_in[:, cols].astype(jnp.float32)
        vf[pl.ds(ROWS, toks), cols] = v_in[:, cols].astype(jnp.float32)
        for block in range(blocks):
            mixed(block * ROWS, ROWS, cols)
        step = jnp.exp(-rate[:, cols])
        state = jnp.zeros((modes, wide * LANES), jnp.float32)
        for t in range(2, toks):
            state = step * state + x[pl.ds(t, 1), cols]
        for i in range(wide):
            ends[at * wide + i] = state[:, i * LANES : (i + 1) * LANES]
        return 0

    lax.fori_loop(0, strips // wide, first_pass, 0)

    around = (members - 1) + (planes - 1)
    pl.semaphore_wait(barrier, around + jnp.where(first_of_plane | last_of_plane, 1, 0))

    for copy in tail_loads:
        copy.wait()

    def halo_copy(device):
        return pltpu.make_async_remote_copy(
            src_ref=tails, dst_ref=halos, send_sem=halo_send, recv_sem=halo_recv,
            device_id={"seq": device}, device_id_type=MESH,
        )

    @pl.when(me < last)
    def _():
        halo_copy(me + 1).start()

    @pl.when(me == 0)
    def _():
        for i in range(3):
            halos[i] = jnp.zeros((ROWS, width), jnp.bfloat16)

    @pl.when(me > 0)
    def _():
        halo_copy(me - 1).wait_recv()

    def patch(strip, _):
        cols = lanes(strip)
        kf[0:ROWS, cols] = halos[0, :, cols].astype(jnp.float32)
        vf[0:ROWS, cols] = halos[1, :, cols].astype(jnp.float32)
        mixed(0, ROWS, cols)
        fade = rate[:, cols]
        first = jnp.exp(-(toks - 1.0) * fade) * x[0:1, cols]
        second = jnp.exp(-(toks - 2.0) * fade) * x[1:2, cols]
        ends[strip] = ends[strip] + first + second
        return 0

    lax.fori_loop(0, strips, patch, 0)

    def up(i):
        return pltpu.make_async_remote_copy(
            src_ref=ends.at[i], dst_ref=got.at[spot], send_sem=up_send.at[i], recv_sem=up_recv.at[spot],
            device_id={"seq": plane * members + i}, device_id_type=MESH,
        )

    for i in range(members):

        @pl.when(spot != i)
        def _():
            up(i).start()

    got[spot] = ends[spot]

    for copy in (res_load, skip_load, q_load):
        copy.wait()

    places = lax.broadcasted_iota(jnp.int32, (ROWS, LANES), 0)

    def second_pass(at, _):
        cols = lanes(at * wide, wide)
        step = jnp.exp(-rate[:, cols])
        state = jnp.zeros((modes, wide * LANES), jnp.float32)
        for t in range(toks):
            if t % ROWS == 0:
                for i in range(wide):
                    held[i, t // ROWS] = state[:, i * LANES : (i + 1) * LANES]
            state = step * state + x[pl.ds(t, 1), cols]
        scale = res[:, cols] * jnp.sqrt(1.0 - jnp.exp(-2.0 * rate[:, cols]))
        qf[pl.ds(0, ROWS), cols] = halos[2, :, cols].astype(jnp.float32)
        qf[pl.ds(ROWS, toks), cols] = q_in[:, cols].astype(jnp.float32)
        for i in range(wide):
            strip = at * wide + i
            mine = lanes(strip)
            later = (places + 1).astype(jnp.float32)
            after = jnp.zeros((ROWS, LANES), jnp.float32)
            for m in range(modes):
                weight = scale[m : m + 1, i * LANES : (i + 1) * LANES]
                table = jnp.exp(-later * rate[pl.ds(m, 1), mine]) * weight
                gain[strip, m] = table
                after = after + table
            now = jnp.sum(scale[:, i * LANES : (i + 1) * LANES], axis=0, keepdims=True)
            now = now + skip[pl.ds(strip, 1), :]
            taper = jnp.where(places == 0, now, pltpu.roll(after, 1, 0))
            near = [taper] + [jnp.where(places >= j, pltpu.roll(taper, j, 0), 0.0) for j in range(1, ROWS)]
            for block in range(blocks):
                total = near[0] * x[pl.ds(block * ROWS, 1), mine]
                for j in range(1, ROWS):
                    total = total + near[j] * x[pl.ds(block * ROWS + j, 1), mine]
                if block > 0:
                    for m in range(modes):
                        total = total + gain[strip, m] * held[i, block, pl.ds(m, 1), :]
                y[pl.ds(block * ROWS, ROWS), mine] = total
        return 0

    lax.fori_loop(0, strips // wide, second_pass, 0)

    for i in range(members):

        @pl.when(spot != i)
        def _():
            pltpu.make_async_remote_copy(
                src_ref=got.at[i], dst_ref=got.at[i], send_sem=up_send.at[i], recv_sem=up_recv.at[i],
                device_id={"seq": me}, device_id_type=MESH,
            ).wait_recv()

    fade = rate[:, lanes(spot)]
    long_step = jnp.exp(-float(toks) * fade)
    total = jnp.zeros((modes, LANES), jnp.float32)
    for i in range(members):
        starts[i] = total
        total = long_step * total + got[i]
    sums[...] = total

    def side(i):
        return pltpu.make_async_remote_copy(
            src_ref=sums, dst_ref=sums_in.at[plane], send_sem=side_send.at[i], recv_sem=side_recv.at[plane],
            device_id={"seq": i * members + spot}, device_id_type=MESH,
        )

    for i in range(1, planes):

        @pl.when(plane < i)
        def _():
            side(i).start()

    def widen(strip, _):
        fade = rate[:, lanes(strip)]
        factor = jnp.exp(-float(ROWS) * fade)
        power = jnp.ones_like(factor)
        for block in range(blocks):
            spread[strip, block] = power
            power = power * factor
        return 0

    lax.fori_loop(0, strips, widen, 0)

    carry[...] = jnp.zeros((modes, LANES), jnp.float32)
    plane_step = jnp.exp(-float(toks * members) * fade)
    for i in range(planes - 1):

        @pl.when(plane > i)
        def _():
            pltpu.make_async_remote_copy(
                src_ref=sums_in.at[i], dst_ref=sums_in.at[i], send_sem=side_send.at[i], recv_sem=side_recv.at[i],
                device_id={"seq": me}, device_id_type=MESH,
            ).wait_recv()
            carry[...] = plane_step * carry[...] + sums_in[i]

    entering = carry[...]
    for i in range(members):
        starts[i] = starts[i] + jnp.exp(-float(toks * i) * fade) * entering

    def down(i):
        return pltpu.make_async_remote_copy(
            src_ref=starts.at[i], dst_ref=starts_in.at[spot], send_sem=down_send.at[i], recv_sem=down_recv.at[spot],
            device_id={"seq": plane * members + i}, device_id_type=MESH,
        )

    for i in range(members):

        @pl.when(spot != i)
        def _():
            down(i).start()

    starts_in[spot] = starts[spot]

    for i in range(members):

        @pl.when(spot != i)
        def _():
            pltpu.make_async_remote_copy(
                src_ref=starts_in.at[i], dst_ref=starts_in.at[i], send_sem=down_send.at[i], recv_sem=down_recv.at[i],
                device_id={"seq": me}, device_id_type=MESH,
            ).wait_recv()

    def last_pass(strip, _):
        cols = lanes(strip)
        entry = starts_in[strip]
        for block in range(blocks):
            held[0, block] = spread[strip, block] * entry
        for block in range(blocks):
            rows = pl.ds(block * ROWS, ROWS)
            total = y[rows, cols]
            for m in range(modes):
                total = total + gain[strip, m] * held[0, block, pl.ds(m, 1), :]
            q_short = short(qf, 0, block * ROWS, ROWS, cols)
            y[rows, cols] = q_short * total.astype(jnp.bfloat16).astype(jnp.float32)
        gated[:, cols] = y[:, cols].astype(jnp.bfloat16)
        return 0

    lax.fori_loop(0, strips, last_pass, 0)

    w_load.wait()
    column = min(256, width)

    def project(at, _):
        cols = pl.ds(pl.multiple_of(at * column, column), column)
        out_ref[:, cols] = jnp.dot(
            gated[...], w_in[:, cols], preferred_element_type=jnp.float32
        ).astype(out_ref.dtype)
        return 0

    lax.fori_loop(0, width // column, project, 0)

    @pl.when(me < last)
    def _():
        halo_copy(me + 1).wait_send()

    for i in range(members):

        @pl.when(spot != i)
        def _():
            up(i).wait_send()
            down(i).wait_send()

    for i in range(1, planes):

        @pl.when(plane < i)
        def _():
            side(i).wait_send()


def body(planes, queries, keys, values, short_taps, decay, residue, skip, w_out):
    toks, width = queries.shape
    modes = decay.shape[1]
    strips = width // LANES
    blocks = toks // ROWS
    wide = min(4, strips)
    f32, bf16 = jnp.float32, jnp.bfloat16
    dma = pltpu.SemaphoreType.DMA
    anywhere = pl.BlockSpec(memory_space=pl.ANY)
    return pl.pallas_call(
        functools.partial(kernel, planes),
        out_shape=jax.ShapeDtypeStruct((toks, width), bf16),
        in_specs=[anywhere] * 8,
        out_specs=pl.BlockSpec(memory_space=pltpu.VMEM),
        scratch_shapes=[
            pltpu.VMEM((toks, width), bf16),
            pltpu.VMEM((toks, width), bf16),
            pltpu.VMEM((toks, width), bf16),
            pltpu.VMEM((3, ROWS, width), bf16),
            pltpu.VMEM((3, ROWS, width), bf16),
            pltpu.VMEM((3, 3, width), f32),
            pltpu.VMEM((modes, width), f32),
            pltpu.VMEM((modes, width), f32),
            pltpu.VMEM((strips, LANES), f32),
            pltpu.VMEM((width, width), bf16),
            pltpu.VMEM((toks + ROWS, width), f32),
            pltpu.VMEM((toks + ROWS, width), f32),
            pltpu.VMEM((toks + ROWS, width), f32),
            pltpu.VMEM((toks, width), f32),
            pltpu.VMEM((toks, width), f32),
            pltpu.VMEM((strips, modes, ROWS, LANES), f32),
            pltpu.VMEM((strips, modes, LANES), f32),
            pltpu.VMEM((strips, modes, LANES), f32),
            pltpu.VMEM((modes, LANES), f32),
            pltpu.VMEM((modes, LANES), f32),
            pltpu.VMEM((planes, modes, LANES), f32),
            pltpu.VMEM((strips, modes, LANES), f32),
            pltpu.VMEM((strips, modes, LANES), f32),
            pltpu.VMEM((wide, blocks, modes, LANES), f32),
            pltpu.VMEM((strips, blocks, modes, LANES), f32),
            pltpu.VMEM((toks, width), bf16),
            dma((11,)),
            dma,
            dma,
            dma((strips,)),
            dma((strips,)),
            dma((planes,)),
            dma((planes,)),
            dma((strips,)),
            dma((strips,)),
        ],
        compiler_params=pltpu.CompilerParams(
            collective_id=0, has_side_effects=True, vmem_limit_bytes=60 * 1024 * 1024
        ),
    )(
        queries, keys, values, short_taps, decay.T, residue.T,
        skip.reshape(strips, LANES), w_out,
    )


def solution(mesh):
    split = P(("rep", "seq"), None)
    placed = (split, split, split, P(), P(), P(), P(), P())

    def run(queries, *rest):
        planes = mesh.shape["seq"] * LANES // queries.shape[1]
        return body(planes, queries, *rest)

    return jax.shard_map(run, mesh=mesh, in_specs=placed, out_specs=split, check_vma=False)
```

```python
import functools
import math

import jax
import jax.numpy as jnp
from jax import lax
from jax.experimental import pallas as pl
from jax.experimental.pallas import tpu as pltpu
from jax.sharding import PartitionSpec as P

MESH = pl.DeviceIdType.MESH
LANES = 128
ROWS = 8


def lanes(strip, count=1):
    return pl.ds(pl.multiple_of(strip * LANES, LANES), count * LANES)


def scratch(planes, toks, width, modes):
    f32, bf16 = jnp.float32, jnp.bfloat16
    strips, blocks = width // LANES, toks // ROWS
    wide = math.isqrt(strips)
    dma = pltpu.SemaphoreType.DMA
    return dict(
        q_in=pltpu.VMEM((toks, width), bf16),
        k_in=pltpu.VMEM((toks, width), bf16),
        v_in=pltpu.VMEM((toks, width), bf16),
        tails=pltpu.VMEM((ROWS, width), bf16),
        halos=pltpu.VMEM((ROWS, width), bf16),
        taps=pltpu.VMEM((3, 3, width), f32),
        rate=pltpu.VMEM((modes, width), f32),
        res=pltpu.VMEM((modes, width), f32),
        skip=pltpu.VMEM((strips, LANES), f32),
        w_in=pltpu.VMEM((width, width), bf16),
        qf=pltpu.VMEM((toks + ROWS, width), f32),
        kf=pltpu.VMEM((toks + ROWS, width), f32),
        vf=pltpu.VMEM((toks + ROWS, width), f32),
        x=pltpu.VMEM((toks, width), f32),
        y=pltpu.VMEM((toks, width), f32),
        gate=pltpu.VMEM((toks, width), f32),
        total=pltpu.VMEM((toks, width), f32),
        gated=pltpu.VMEM((2, toks, wide * LANES), bf16),
        gain=pltpu.VMEM((strips, modes, ROWS, LANES), f32),
        near=pltpu.VMEM((strips, ROWS, ROWS, LANES), f32),
        ahead=pltpu.VMEM((strips, LANES), f32),
        drop=pltpu.VMEM((strips, modes, LANES), f32),
        held=pltpu.VMEM((strips, blocks, modes, LANES), f32),
        edges=pltpu.VMEM((strips, ROWS, LANES), bf16),
        edges_in=pltpu.VMEM((strips, ROWS, LANES), bf16),
        rows_in=pltpu.VMEM((strips * ROWS, LANES), f32),
        heads=pltpu.VMEM((2, strips, LANES), f32),
        shift=pltpu.VMEM((strips, modes, LANES), f32),
        ends=pltpu.VMEM((strips, modes, LANES), f32),
        got=pltpu.VMEM((strips, modes, LANES), f32),
        sums=pltpu.VMEM((modes + ROWS, LANES), f32),
        carry=pltpu.VMEM((2, modes, LANES), f32),
        sums_in=pltpu.VMEM((planes, modes + ROWS, LANES), f32),
        starts=pltpu.VMEM((strips, modes, LANES), f32),
        starts_in=pltpu.VMEM((strips, modes, LANES), f32),
        load_sem=dma((15,)),
        halo_send=dma,
        halo_recv=dma,
        edge_send=dma((strips,)),
        edge_recv=dma((strips,)),
        up_send=dma((strips,)),
        up_recv=dma((strips,)),
        side_send=dma((planes,)),
        side_recv=dma((planes,)),
        down_send=dma((strips,)),
        down_recv=dma((strips,)),
        ready=pltpu.SemaphoreType.REGULAR((planes + 1,)),
    )


def kernel(planes, names, q_hbm, k_hbm, v_hbm, taps_hbm, rate_hbm, res_hbm, skip_hbm, w_hbm, out_ref, *refs):
    s = dict(zip(names, refs, strict=True))
    q_in, k_in, v_in, tails, halos, taps = (s[n] for n in ("q_in", "k_in", "v_in", "tails", "halos", "taps"))
    rate, res, skip, w_in, qf, kf, vf, x = (s[n] for n in ("rate", "res", "skip", "w_in", "qf", "kf", "vf", "x"))
    y, gate, total, gated, gain, near, ahead, drop = (
        s[n] for n in ("y", "gate", "total", "gated", "gain", "near", "ahead", "drop")
    )
    held, edges, edges_in, rows_in, heads = (s[n] for n in ("held", "edges", "edges_in", "rows_in", "heads"))
    shift, ends, got, sums, carry = (s[n] for n in ("shift", "ends", "got", "sums", "carry"))
    sums_in, starts, starts_in = (s[n] for n in ("sums_in", "starts", "starts_in"))

    f32, bf16 = jnp.float32, jnp.bfloat16
    toks, width = q_hbm.shape
    modes = rate_hbm.shape[0]
    strips, blocks = width // LANES, toks // ROWS
    members, wide = strips, math.isqrt(strips)
    chunk = wide * LANES
    half = strips // 2
    me = lax.axis_index("seq")
    plane, spot = me // members, me % members
    spot_y, spot_x = spot // wide, spot % wide
    first_plane = plane * members
    last = planes * members - 1

    def load(source, target, at):
        copy = pltpu.make_async_copy(source, target, s["load_sem"].at[at])
        copy.start()
        return copy

    rate_load = load(rate_hbm, rate, 3)
    taps_load = load(taps_hbm, taps, 4)
    k_loads, v_loads = [], []
    for c in range(2):
        cols = pl.ds(c * half * LANES, half * LANES)
        k_loads.append(load(k_hbm.at[:, cols], k_in.at[:, cols], 11 + 2 * c))
        v_loads.append(load(v_hbm.at[:, cols], v_in.at[:, cols], 12 + 2 * c))
    res_load = load(res_hbm, res, 5)
    skip_load = load(skip_hbm, skip, 6)
    q_load = load(q_hbm, q_in, 7)
    w_load = load(w_hbm, w_in, 8)

    barrier = pltpu.get_barrier_semaphore()

    def greet(device):
        pl.semaphore_signal(barrier, inc=1, device_id={"seq": device}, device_id_type=MESH)

    for i in range(members):

        @pl.when(spot != i)
        def _():
            greet(first_plane + i)

    for i in range(1, planes):

        @pl.when(plane < i)
        def _():
            greet(i * members + spot)

    after_end = (plane > 0) & (spot == 0)
    before_start = (plane < planes - 1) & (spot == members - 1)

    @pl.when(before_start)
    def _():
        greet(me + 1)

    def short(source, kind, start, count, cols):
        rows = [source[pl.ds(ROWS + start - lag, count), cols] for lag in range(3)]
        result = taps[kind, 0:1, cols] * rows[0] + taps[kind, 1:2, cols] * rows[1]
        return result + taps[kind, 2:3, cols] * rows[2]

    def mixed(start, count, cols):
        product = short(kf, 1, start, count, cols) * short(vf, 2, start, count, cols)
        x[pl.ds(start, count), cols] = product.astype(bf16).astype(f32)

    def first_pass(at):
        size = half * LANES
        cols = pl.ds(at * size, size)
        kf[0:ROWS, cols] = jnp.zeros((ROWS, size), f32)
        vf[0:ROWS, cols] = jnp.zeros((ROWS, size), f32)
        kf[pl.ds(ROWS, toks), cols] = k_in[:, cols].astype(f32)
        vf[pl.ds(ROWS, toks), cols] = v_in[:, cols].astype(f32)
        for block in range(blocks):
            mixed(block * ROWS, ROWS, cols)
        step = jnp.exp(-rate[:, cols])
        state = jnp.zeros((modes, size), f32)
        for t in range(2, toks):
            if t % ROWS == 0:
                for i in range(half):
                    held[at * half + i, t // ROWS] = state[:, i * LANES : (i + 1) * LANES]
            state = step * state + x[pl.ds(t, 1), cols]
        for i in range(half):
            ends[at * half + i] = state[:, i * LANES : (i + 1) * LANES]

    def remote(source, target, send, recv, device):
        return pltpu.make_async_remote_copy(
            src_ref=source, dst_ref=target, send_sem=send, recv_sem=recv,
            device_id={"seq": device}, device_id_type=MESH,
        )

    def edge(i):
        return remote(edges.at[i], edges_in.at[spot], s["edge_send"].at[i], s["edge_recv"].at[spot], first_plane + i)

    def up(i):
        return remote(ends.at[i], got.at[spot], s["up_send"].at[i], s["up_recv"].at[spot], first_plane + i)

    def side(i):
        return remote(sums, sums_in.at[plane], s["side_send"].at[i], s["side_recv"].at[plane], i * members + spot)

    def down(i):
        return remote(starts.at[i], starts_in.at[spot], s["down_send"].at[i], s["down_recv"].at[spot], first_plane + i)

    def halo(device):
        return remote(tails, halos, s["halo_send"], s["halo_recv"], device)

    rate_load.wait()
    taps_load.wait()
    k_loads[0].wait()
    v_loads[0].wait()
    first_pass(0)
    k_loads[1].wait()
    v_loads[1].wait()
    first_pass(1)
    for i in range(strips):
        cols = lanes(i)
        for j, ref in enumerate((k_in, v_in)):
            edges[i, 2 * j : 2 * j + 2] = ref[0:2, cols]
            edges[i, 4 + 2 * j : 6 + 2 * j] = ref[toks - 2 : toks, cols]
    pl.semaphore_wait(barrier, members - 1 + plane + jnp.where(after_end, 1, 0))
    def ring(d):
        return min(d, wide - d)

    hops = [(dy, dx) for dy in range(wide) for dx in range(wide) if dy + dx > 0]
    hops = sorted(hops, key=lambda d: -ring(d[0]) - ring(d[1]))
    peers = [lax.rem(spot_y + dy, wide) * wide + lax.rem(spot_x + dx, wide) for dy, dx in hops]
    for i in peers:
        edge(i).start()
        up(i).start()

    def hail(device, at):
        pl.semaphore_signal(s["ready"].at[at], inc=1, device_id={"seq": device}, device_id_type=MESH)

    for i in range(planes - 1):

        @pl.when(plane > i)
        def _():
            hail(i * members + spot, plane)

    @pl.when(after_end)
    def _():
        hail(me - 1, planes)

    got[spot] = ends[spot]
    edges_in[spot] = edges[spot]

    @pl.when(me == 0)
    def _():
        halos[...] = jnp.zeros((ROWS, width), bf16)

    for copy in (q_load, res_load, skip_load):
        copy.wait()

    for i, ref in enumerate((k_in, v_in, q_in)):
        tails[2 * i : 2 * i + 2] = ref[toks - 2 : toks]

    @pl.when(spot < members - 1)
    def _():
        halo(me + 1).start()

    places = lax.broadcasted_iota(jnp.int32, (ROWS, LANES), 0)
    later = (places + 1).astype(f32)

    def tabulate(strip, _):
        mine = lanes(strip)
        fade = rate[:, mine]
        scale = res[:, mine] * jnp.sqrt(1.0 - jnp.exp(-2.0 * fade))
        drop[strip] = jnp.exp(-float(ROWS) * fade)
        ahead[pl.ds(strip, 1), :] = jnp.sum(scale * jnp.exp(fade), axis=0, keepdims=True)
        after = jnp.zeros((ROWS, LANES), f32)
        for m in range(modes):
            table = jnp.exp(-later * rate[pl.ds(m, 1), mine]) * scale[m : m + 1]
            gain[strip, m] = table
            after = after + table
        now = jnp.sum(scale, axis=0, keepdims=True) + skip[pl.ds(strip, 1), :]
        taper = jnp.where(places == 0, now, pltpu.roll(after, 1, 0))
        near[strip, 0] = taper
        for j in range(1, ROWS):
            near[strip, j] = jnp.where(places >= j, pltpu.roll(taper, j, 0), 0.0)
        return 0

    lax.fori_loop(0, strips, tabulate, 0)
    def gates(strip, _):
        cols = lanes(strip)
        qf[pl.ds(ROWS, toks), cols] = q_in[:, cols].astype(f32)
        for block in range(1, blocks):
            gate[pl.ds(block * ROWS, ROWS), cols] = short(qf, 0, block * ROWS, ROWS, cols)
        return 0

    lax.fori_loop(0, strips, gates, 0)
    def local(strip, _):
        mine = lanes(strip)
        for block in range(blocks):
            parts = [near[strip, j] * x[pl.ds(block * ROWS + j, 1), mine] for j in range(0 if block else 2, ROWS)]
            if block > 0:
                parts += [gain[strip, m] * held[strip, block, pl.ds(m, 1), :] for m in range(modes)]
            y[pl.ds(block * ROWS, ROWS), mine] = functools.reduce(jnp.add, parts)
        return 0

    lax.fori_loop(0, strips, local, 0)
    for i in range(members):

        @pl.when(spot != i)
        def _():
            remote(edges_in.at[i], edges_in.at[i], s["edge_send"].at[i], s["edge_recv"].at[i], me).wait_recv()

    mine = lanes(spot)
    fade = rate[:, mine]
    for i in range(members):
        rows_in[i * ROWS : (i + 1) * ROWS] = edges_in[i].astype(f32)
    sums[modes : modes + 4] = rows_in[0:4]
    sums[modes + 4 : modes + 8] = rows_in[members * ROWS - 4 : members * ROWS]

    def two_inputs(head, tail):
        pairs = []
        for kind, offset in ((1, 0), (2, 2)):
            now, then, older, old = head(offset), head(offset + 1), tail(4 + offset), tail(5 + offset)
            t = [taps[kind, lag : lag + 1, mine] for lag in range(3)]
            pairs.append(((t[0] * now + t[1] * old) + t[2] * older, (t[0] * then + t[1] * now) + t[2] * old))
        (k_first, k_second), (v_first, v_second) = pairs
        return [(k * v).astype(bf16).astype(f32) for k, v in ((k_first, v_first), (k_second, v_second))]

    fall = [jnp.exp(-(toks - 1.0 - i) * fade) for i in range(2)]
    rise = [jnp.exp((1.0 + i) * fade) for i in range(2)]
    rest = members - 1
    inner = two_inputs(
        lambda r: rows_in[pl.ds(ROWS + r, rest, stride=ROWS), :], lambda r: rows_in[pl.ds(r, rest, stride=ROWS), :]
    )
    for i, rows in enumerate(inner):
        heads[i, 0:rest] = rows
    for i in range(rest):
        shift[i] = fall[0] * heads[0, i : i + 1] + fall[1] * heads[1, i : i + 1]
    for i in range(members):

        @pl.when(spot != i)
        def _():
            remote(got.at[i], got.at[i], s["up_send"].at[i], s["up_recv"].at[i], me).wait_recv()

    long_step = jnp.exp(-float(toks) * fade)
    running = jnp.zeros((modes, LANES), f32)
    for i in range(members):
        starts[i] = running
        running = long_step * running + got[i]
        if i > 0:
            running = running + shift[i - 1]
    sums[0:modes] = running

    for i in range(1, planes):

        @pl.when(plane < i)
        def _():
            pl.semaphore_wait(s["ready"].at[i], 1)
            side(i).start()

    @pl.when(before_start)
    def _():
        pl.semaphore_wait(s["ready"].at[planes], 1)
        halo(me + 1).start()

    sums_in[plane] = sums[...]
    for i in range(rest):
        starts[i + 1] = starts[i + 1] + (rise[0] * heads[0, i : i + 1] + rise[1] * heads[1, i : i + 1])
    carry[0] = jnp.zeros((modes, LANES), f32)
    rest_step = jnp.exp(-float(toks * rest) * fade)
    powers = [jnp.exp(-float(toks * i) * fade) for i in range(rest)]
    for i in range(planes):

        @pl.when(plane >= i)
        def _():
            if i < planes - 1:

                @pl.when(plane > i)
                def _():
                    remote(sums_in.at[i], sums_in.at[i], s["side_send"].at[i], s["side_recv"].at[i], me).wait_recv()

            def row(at, r):
                return sums_in[at, modes + r : modes + r + 1, :]

            none = jnp.zeros((1, LANES), f32)
            x_first, x_second = two_inputs(lambda r: row(i, r), lambda r: row(i - 1, r) if i else none)
            moved = long_step * carry[0] + (fall[0] * x_first + fall[1] * x_second)

            @pl.when(plane == i)
            def _():
                starts[0] = carry[0] + (rise[0] * x_first + rise[1] * x_second)
                carry[1] = moved

            @pl.when(plane > i)
            def _():
                carry[0] = rest_step * moved + sums_in[i, 0:modes]

    moved = carry[1]
    for i in range(rest):
        starts[i + 1] = starts[i + 1] + powers[i] * moved

    for i in peers:
        down(i).start()

    starts_in[spot] = starts[spot]
    @pl.when(me > 0)
    def _():
        halo(me - 1).wait_recv()

    def patch(strip, _):
        cols = lanes(strip)
        kf[ROWS - 2 : ROWS, cols] = halos[0:2, cols].astype(f32)
        vf[ROWS - 2 : ROWS, cols] = halos[2:4, cols].astype(f32)
        qf[ROWS - 2 : ROWS, cols] = halos[4:6, cols].astype(f32)
        product = (short(kf, 1, 0, ROWS, cols) * short(vf, 2, 0, ROWS, cols)).astype(bf16).astype(f32)
        direct = jnp.where(places < 2, skip[pl.ds(strip, 1), :] * product, 0.0)
        extra = jnp.where(places == 0, ahead[pl.ds(strip, 1), :] * product[1:2], 0.0)
        y[0:ROWS, cols] = y[0:ROWS, cols] + (direct - extra)
        gate[0:ROWS, cols] = short(qf, 0, 0, ROWS, cols)
        return 0

    lax.fori_loop(0, strips, patch, 0)
    column = min(256, width)

    def fetch(at):
        for i in range(wide):
            strip = at * wide + i

            @pl.when(spot != strip)
            def _():
                remote(
                    starts_in.at[strip], starts_in.at[strip], s["down_send"].at[strip], s["down_recv"].at[strip], me
                ).wait_recv()

    def finish(at, slot):
        for i in range(wide):
            strip = at * wide + i
            cols = lanes(strip)
            terms = [gain[strip, m] * starts_in[strip, pl.ds(m, 1), :] for m in range(modes)]
            fades = [jnp.broadcast_to(drop[strip, pl.ds(m, 1), :], (ROWS, LANES)) for m in range(modes)]
            for block in range(blocks):
                rows = pl.ds(block * ROWS, ROWS)
                result = y[rows, cols]
                for m in range(modes):
                    result = result + terms[m]
                if block < blocks - 1:
                    terms = [term * fade for term, fade in zip(terms, fades, strict=True)]
                x[rows, cols] = gate[rows, cols] * result.astype(bf16).astype(f32)
            gated[slot, :, i * LANES : (i + 1) * LANES] = x[:, cols].astype(bf16)

    def project(at, slot, begins, stops):
        rows = pl.ds(pl.multiple_of(at * chunk, chunk), chunk)
        for n in range(width // column):
            cols = slice(n * column, (n + 1) * column)
            part = jnp.dot(gated[slot], w_in[rows, cols], preferred_element_type=f32)
            if not begins:
                part = part + total[:, cols]
            if stops:
                out_ref[:, cols] = part.astype(out_ref.dtype)
            else:
                total[:, cols] = part

    order = sorted(range(wide), key=ring)
    turns = [lax.rem(spot_y + d, wide) for d in order]
    fetch(turns[0])
    finish(turns[0], 0)
    w_load.wait()
    for j in range(1, wide):
        fetch(turns[j])
        project(turns[j - 1], (j - 1) % 2, j == 1, False)
        finish(turns[j], j % 2)
    project(turns[wide - 1], (wide - 1) % 2, wide == 1, True)
    @pl.when(me < last)
    def _():
        halo(me + 1).wait_send()

    for i in peers:
        edge(i).wait_send()
        up(i).wait_send()
        down(i).wait_send()

    for i in range(1, planes):

        @pl.when(plane < i)
        def _():
            side(i).wait_send()


def body(planes, queries, keys, values, short_taps, decay, residue, skip, w_out):
    toks, width = queries.shape
    modes = decay.shape[1]
    held = scratch(planes, toks, width, modes)
    outside = pl.BlockSpec(memory_space=pltpu.HBM)
    return pl.pallas_call(
        functools.partial(kernel, planes, tuple(held)),
        out_shape=jax.ShapeDtypeStruct((toks, width), jnp.bfloat16),
        in_specs=[outside] * 8,
        out_specs=pl.BlockSpec(memory_space=pltpu.VMEM),
        scratch_shapes=list(held.values()),
        compiler_params=pltpu.CompilerParams(
            collective_id=0, has_side_effects=True, vmem_limit_bytes=48 * 1024 * 1024
        ),
    )(
        *(
            pltpu.with_memory_space_constraint(value, pltpu.HBM)
            for value in (
                queries, keys, values, short_taps, decay.T, residue.T,
                skip.reshape(width // LANES, LANES), w_out,
            )
        )
    )


def solution(mesh):
    split = P(("rep", "seq"), None)
    placed = (split, split, split, P(), P(), P(), P(), P())

    def run(queries, *rest):
        planes = mesh.shape["seq"] * LANES // queries.shape[1]
        return body(planes, queries, *rest)

    return jax.shard_map(run, mesh=mesh, in_specs=placed, out_specs=split, check_vma=False)
```

```python
import functools
import math

import jax
import jax.numpy as jnp
from jax import lax
from jax.experimental import pallas as pl
from jax.experimental.pallas import tpu as pltpu
from jax.sharding import PartitionSpec as P

MESH = pl.DeviceIdType.MESH
LANES = 128
ROWS = 8


def lanes(strip, count=1):
    return pl.ds(pl.multiple_of(strip * LANES, LANES), count * LANES)


def scratch(planes, toks, width, modes):
    f32, bf16 = jnp.float32, jnp.bfloat16
    strips, blocks = width // LANES, toks // ROWS
    wide = math.isqrt(strips)
    dma = pltpu.SemaphoreType.DMA
    return dict(
        q_in=pltpu.VMEM((toks, width), bf16),
        kv_in=pltpu.VMEM((2, toks, width), bf16),
        tails=pltpu.VMEM((ROWS, width), bf16),
        halos=pltpu.VMEM((ROWS, width), bf16),
        taps=pltpu.VMEM((3, 3, width), f32),
        modal=pltpu.VMEM((2, modes, width), f32),
        skip=pltpu.VMEM((strips, LANES), f32),
        w_in=pltpu.VMEM((width, width), bf16),
        qf=pltpu.VMEM((toks + ROWS, width), f32),
        kv=pltpu.VMEM((strips, 2 * (toks + ROWS), LANES), f32),
        x=pltpu.VMEM((toks, width), f32),
        y=pltpu.VMEM((toks, width), f32),
        gate=pltpu.VMEM((toks, width), f32),
        total=pltpu.VMEM((toks, width), f32),
        gated=pltpu.VMEM((2, toks, wide * LANES), bf16),
        gain=pltpu.VMEM((strips, modes, ROWS, LANES), f32),
        near=pltpu.VMEM((strips, ROWS, ROWS, LANES), f32),
        ahead=pltpu.VMEM((strips, LANES), f32),
        drop=pltpu.VMEM((strips, modes, LANES), f32),
        held=pltpu.VMEM((strips, blocks, modes, LANES), f32),
        edges=pltpu.VMEM((strips, ROWS, LANES), bf16),
        edges_in=pltpu.VMEM((strips, ROWS, LANES), bf16),
        rows_in=pltpu.VMEM((strips * ROWS, LANES), f32),
        heads=pltpu.VMEM((2, strips, LANES), f32),
        shift=pltpu.VMEM((strips, modes, LANES), f32),
        ends=pltpu.VMEM((strips, modes, LANES), f32),
        got=pltpu.VMEM((strips, modes, LANES), f32),
        sums=pltpu.VMEM((modes + ROWS, LANES), f32),
        carry=pltpu.VMEM((2, modes, LANES), f32),
        sums_in=pltpu.VMEM((planes, modes + ROWS, LANES), f32),
        starts=pltpu.VMEM((strips, modes, LANES), f32),
        starts_in=pltpu.VMEM((strips, modes, LANES), f32),
        load_sem=dma((7,)),
        halo_send=dma,
        halo_recv=dma,
        edge_send=dma,
        edge_recv=dma,
        up_send=dma,
        up_recv=dma,
        side_send=dma((planes - 1,)),
        side_recv=dma((planes - 1,)),
        down_send=dma,
        down_recv=dma((wide + 1,)),
        ready=pltpu.SemaphoreType.REGULAR((planes,)),
    )


def kernel(planes, names, q_hbm, k_hbm, v_hbm, taps_hbm, rate_hbm, res_hbm, skip_hbm, w_hbm, out_ref, *refs):
    s = dict(zip(names, refs, strict=True))
    q_in, kv_in, tails, halos, modal = (s[n] for n in ("q_in", "kv_in", "tails", "halos", "modal"))
    taps, skip, w_in, qf, kv, x = (s[n] for n in ("taps", "skip", "w_in", "qf", "kv", "x"))
    k_in, v_in = kv_in.at[0], kv_in.at[1]
    rate, res = modal.at[0], modal.at[1]
    y, gate, total, gated, gain, near, ahead, drop = (
        s[n] for n in ("y", "gate", "total", "gated", "gain", "near", "ahead", "drop")
    )
    held, edges, edges_in, rows_in, heads = (s[n] for n in ("held", "edges", "edges_in", "rows_in", "heads"))
    shift, ends, got, sums, carry = (s[n] for n in ("shift", "ends", "got", "sums", "carry"))
    sums_in, starts, starts_in = (s[n] for n in ("sums_in", "starts", "starts_in"))

    f32, bf16 = jnp.float32, jnp.bfloat16
    toks, width = q_hbm.shape
    modes = rate_hbm.shape[0]
    strips, blocks = width // LANES, toks // ROWS
    members, wide = strips, math.isqrt(strips)
    half = strips // 2
    me = lax.axis_index("seq")
    plane, spot = me // members, me % members
    spot_y, spot_x = spot // wide, spot % wide
    first_plane = plane * members
    last = planes * members - 1

    def load(source, target, at):
        copy = pltpu.make_async_copy(source, target, s["load_sem"].at[at])
        copy.start()
        return copy

    load(rate_hbm, rate, 0)
    load(res_hbm, res, 0)
    taps_load = load(taps_hbm, taps, 1)
    halves = [pl.ds(c * half * LANES, half * LANES) for c in range(2)]
    for c, cols in enumerate(halves):
        load(k_hbm.at[:, cols], k_in.at[:, cols], 2 + c)
        load(v_hbm.at[:, cols], v_in.at[:, cols], 2 + c)

    barrier = pltpu.get_barrier_semaphore()

    def greet(device):
        pl.semaphore_signal(barrier, inc=1, device_id={"seq": device}, device_id_type=MESH)

    def ring(d):
        return min(d, wide - d)

    hops = [(dy, dx) for dy in range(wide) for dx in range(wide) if dy + dx > 0]
    hops = sorted(hops, key=lambda d: -ring(d[0]) - ring(d[1]))
    peers = [lax.rem(spot_y + dy, wide) * wide + lax.rem(spot_x + dx, wide) for dy, dx in hops]
    for i in peers:
        greet(first_plane + i)

    for i in range(1, planes):

        @pl.when(plane < i)
        def _():
            greet(i * members + spot)

    closing = (spot == members - 1) & (plane < planes - 1)
    opening = (spot == 0) & (plane > 0)

    @pl.when(closing)
    def _():
        greet(me + 1)

    skip_load = load(skip_hbm, skip, 4)
    q_load = load(q_hbm, q_in, 5)
    w_load = load(w_hbm, w_in, 6)

    def arrive(ref, sem):
        pltpu.make_async_copy(ref, ref, sem).wait()

    def short(source, kind, start, count, cols):
        rows = [source[pl.ds(ROWS + start - lag, count), cols] for lag in range(3)]
        result = taps[kind, 0:1, cols] * rows[0] + taps[kind, 1:2, cols] * rows[1]
        return result + taps[kind, 2:3, cols] * rows[2]

    def paired(strip, kind, start):
        return kv[strip, pl.ds(2 * (ROWS + start) + kind - 1, ROWS, stride=2), :]

    def mixed(strip, start, weights):
        parts = []
        for kind in (1, 2):
            rows = [paired(strip, kind, start - lag) for lag in range(3)]
            t = weights[kind]
            parts.append((t[0] * rows[0] + t[1] * rows[1]) + t[2] * rows[2])
        return (parts[0] * parts[1]).astype(bf16).astype(f32)

    def taps_of(cols):
        return [None] + [[taps[kind, lag : lag + 1, cols] for lag in range(3)] for kind in (1, 2)]

    def first_pass(at):
        strips_now = range(at * half, (at + 1) * half)
        for strip in strips_now:
            cols = pl.ds(strip * LANES, LANES)
            weights = taps_of(cols)
            kv[strip, 0 : 2 * ROWS] = jnp.zeros((2 * ROWS, LANES), f32)
            for kind, ref in ((1, k_in), (2, v_in)):
                kv[strip, pl.ds(2 * ROWS + kind - 1, toks, stride=2), :] = ref[:, cols].astype(f32)
            for block in range(blocks):
                x[pl.ds(block * ROWS, ROWS), cols] = mixed(strip, block * ROWS, weights)
        steps = [jnp.exp(-rate[:, pl.ds(strip * LANES, LANES)]) for strip in strips_now]
        states = [jnp.zeros((modes, LANES), f32) for _ in strips_now]
        for t in range(2, toks):
            if t % ROWS == 0:
                for strip, state in zip(strips_now, states, strict=True):
                    held[strip, t // ROWS] = state
            rows = [x[pl.ds(t, 1), pl.ds(strip * LANES, LANES)] for strip in strips_now]
            states = [step * state + row for step, state, row in zip(steps, states, rows, strict=True)]
        for strip, state in zip(strips_now, states, strict=True):
            ends[strip] = state

    def remote(source, target, send, recv, device):
        return pltpu.make_async_remote_copy(
            src_ref=source, dst_ref=target, send_sem=send, recv_sem=recv,
            device_id={"seq": device}, device_id_type=MESH,
        )

    def edge(i):
        return remote(edges.at[i], edges_in.at[spot], s["edge_send"], s["edge_recv"], first_plane + i)

    def up(i):
        return remote(ends.at[i], got.at[spot], s["up_send"], s["up_recv"], first_plane + i)

    def side(i):
        return remote(
            sums, sums_in.at[plane], s["side_send"].at[i - 1], s["side_recv"].at[plane], i * members + spot
        )

    def down(i, group):
        return remote(starts.at[i], starts_in.at[spot], s["down_send"], s["down_recv"].at[group], first_plane + i)

    def halo(device):
        return remote(tails, halos, s["halo_send"], s["halo_recv"], device)

    arrive(modal, s["load_sem"].at[0])
    taps_load.wait()
    arrive(kv_in.at[:, :, halves[0]], s["load_sem"].at[2])
    first_pass(0)
    arrive(kv_in.at[:, :, halves[1]], s["load_sem"].at[3])
    first_pass(1)
    for i in range(strips):
        cols = lanes(i)
        for j, ref in enumerate((k_in, v_in)):
            edges[i, 2 * j : 2 * j + 2] = ref[0:2, cols]
            edges[i, 4 + 2 * j : 6 + 2 * j] = ref[toks - 2 : toks, cols]
    pl.semaphore_wait(barrier, members - 1 + plane + jnp.where(opening, 1, 0))
    for i in peers:
        edge(i).start()
        up(i).start()

    def hail(device, at):
        pl.semaphore_signal(s["ready"].at[at], inc=1, device_id={"seq": device}, device_id_type=MESH)

    for i in range(planes - 1):

        @pl.when(plane > i)
        def _():
            hail(i * members + spot, plane - 1)

    @pl.when(opening)
    def _():
        hail(me - 1, planes - 1)

    got[spot] = ends[spot]
    edges_in[spot] = edges[spot]

    @pl.when(me == 0)
    def _():
        halos[...] = jnp.zeros((ROWS, width), bf16)

    q_load.wait()
    skip_load.wait()

    for i, ref in enumerate((k_in, v_in, q_in)):
        tails[2 * i : 2 * i + 2] = ref[toks - 2 : toks]

    @pl.when(spot < members - 1)
    def _():
        halo(me + 1).start()

    places = lax.broadcasted_iota(jnp.int32, (ROWS, LANES), 0)
    later = (places + 1).astype(f32)

    def tabulate(strip, _):
        mine = lanes(strip)
        fade = rate[:, mine]
        scale = res[:, mine] * jnp.sqrt(1.0 - jnp.exp(-2.0 * fade))
        drop[strip] = jnp.exp(-float(ROWS) * fade)
        ahead[pl.ds(strip, 1), :] = jnp.sum(scale * jnp.exp(fade), axis=0, keepdims=True)
        after = jnp.zeros((ROWS, LANES), f32)
        for m in range(modes):
            table = jnp.exp(-later * rate[pl.ds(m, 1), mine]) * scale[m : m + 1]
            gain[strip, m] = table
            after = after + table
        now = jnp.sum(scale, axis=0, keepdims=True) + skip[pl.ds(strip, 1), :]
        taper = jnp.where(places == 0, now, pltpu.roll(after, 1, 0))
        near[strip, 0] = taper
        for j in range(1, ROWS):
            near[strip, j] = jnp.where(places >= j, pltpu.roll(taper, j, 0), 0.0)
        return 0

    lax.fori_loop(0, strips, tabulate, 0)
    def gates(strip, _):
        cols = lanes(strip)
        qf[pl.ds(ROWS, toks), cols] = q_in[:, cols].astype(f32)
        for block in range(1, blocks):
            gate[pl.ds(block * ROWS, ROWS), cols] = short(qf, 0, block * ROWS, ROWS, cols)
        return 0

    lax.fori_loop(0, strips, gates, 0)
    def local(strip, _):
        mine = lanes(strip)
        for block in range(blocks):
            parts = [near[strip, j] * x[pl.ds(block * ROWS + j, 1), mine] for j in range(0 if block else 2, ROWS)]
            if block > 0:
                parts += [gain[strip, m] * held[strip, block, pl.ds(m, 1), :] for m in range(modes)]
            y[pl.ds(block * ROWS, ROWS), mine] = functools.reduce(jnp.add, parts)
        return 0

    early = strips * 3 // 4
    lax.fori_loop(0, early, local, 0)
    others = pl.ds(0, members - 1)
    arrive(edges_in.at[others], s["edge_recv"])
    mine = lanes(spot)
    fade = rate[:, mine]
    for i in range(members):
        rows_in[i * ROWS : (i + 1) * ROWS] = edges_in[i].astype(f32)
    sums[modes : modes + 4] = rows_in[0:4]
    sums[modes + 4 : modes + 8] = rows_in[members * ROWS - 4 : members * ROWS]

    def two_inputs(head, tail):
        pairs = []
        for kind, offset in ((1, 0), (2, 2)):
            now, then, older, old = head(offset), head(offset + 1), tail(4 + offset), tail(5 + offset)
            t = [taps[kind, lag : lag + 1, mine] for lag in range(3)]
            pairs.append(((t[0] * now + t[1] * old) + t[2] * older, (t[0] * then + t[1] * now) + t[2] * old))
        (k_first, k_second), (v_first, v_second) = pairs
        return [(k * v).astype(bf16).astype(f32) for k, v in ((k_first, v_first), (k_second, v_second))]

    fall = [jnp.exp(-(toks - 1.0 - i) * fade) for i in range(2)]
    rise = [jnp.exp((1.0 + i) * fade) for i in range(2)]
    rest = members - 1
    inner = two_inputs(
        lambda r: rows_in[pl.ds(ROWS + r, rest, stride=ROWS), :], lambda r: rows_in[pl.ds(r, rest, stride=ROWS), :]
    )
    for i, rows in enumerate(inner):
        heads[i, 0:rest] = rows
    for i in range(rest):
        shift[i] = fall[0] * heads[0, i : i + 1] + fall[1] * heads[1, i : i + 1]
    arrive(got.at[others], s["up_recv"])
    long_step = jnp.exp(-float(toks) * fade)
    running = jnp.zeros((modes, LANES), f32)
    for i in range(members):
        starts[i] = running
        running = long_step * running + got[i]
        if i > 0:
            running = running + shift[i - 1]
    sums[0:modes] = running

    def send_side(i):
        pl.semaphore_wait(s["ready"].at[i - 1], 1)
        side(i).start()

    for i in range(1, planes):

        @pl.when(((plane > 0) & (plane < i)) | (plane == i - 1))
        def _():
            send_side(i)

    lax.fori_loop(early, strips, local, 0)
    @pl.when(closing)
    def _():
        pl.semaphore_wait(s["ready"].at[planes - 1], 1)
        halo(me + 1).start()

    sums_in[plane] = sums[...]
    for i in range(rest):
        starts[i + 1] = starts[i + 1] + (rise[0] * heads[0, i : i + 1] + rise[1] * heads[1, i : i + 1])
    carry[0] = jnp.zeros((modes, LANES), f32)
    rest_step = jnp.exp(-float(toks * rest) * fade)
    powers = [jnp.exp(-float(toks * i) * fade) for i in range(rest)]
    for i in range(planes):

        @pl.when(plane >= i)
        def _():
            if i < planes - 1:

                @pl.when(plane > i)
                def _():
                    arrive(sums_in.at[i], s["side_recv"].at[i])

            def row(at, r):
                return sums_in[at, modes + r : modes + r + 1, :]

            none = jnp.zeros((1, LANES), f32)
            x_first, x_second = two_inputs(lambda r: row(i, r), lambda r: row(i - 1, r) if i else none)
            moved = long_step * carry[0] + (fall[0] * x_first + fall[1] * x_second)

            @pl.when(plane == i)
            def _():
                starts[0] = carry[0] + (rise[0] * x_first + rise[1] * x_second)
                carry[1] = moved

            @pl.when(plane > i)
            def _():
                carry[0] = rest_step * moved + sums_in[i, 0:modes]

    moved = carry[1]
    for i in range(rest):
        starts[i + 1] = starts[i + 1] + powers[i] * moved

    reach = sorted(range(wide), key=ring)
    pair = 2
    for i, (dy, dx) in zip(peers, hops, strict=True):
        group = reach.index((wide - dy) % wide)
        if group == wide - 1:
            across = lax.rem(spot_x // pair - lax.rem(spot_x + dx, wide) // pair + wide, wide // pair)
            group = group + across
        down(i, group).start()

    @pl.when(plane == 0)
    def _():
        for i in range(2, planes):
            send_side(i)

    starts_in[spot] = starts[spot]
    @pl.when(me > 0)
    def _():
        arrive(halos, s["halo_recv"])

    def patch(strip, _):
        cols = lanes(strip)
        for kind in (1, 2):
            kv[strip, pl.ds(2 * (ROWS - 2) + kind - 1, 2, stride=2), :] = halos[
                2 * kind - 2 : 2 * kind, cols
            ].astype(f32)
        qf[ROWS - 2 : ROWS, cols] = halos[4:6, cols].astype(f32)
        product = mixed(strip, 0, taps_of(cols))
        direct = jnp.where(places < 2, skip[pl.ds(strip, 1), :] * product, 0.0)
        extra = jnp.where(places == 0, ahead[pl.ds(strip, 1), :] * product[1:2], 0.0)
        y[0:ROWS, cols] = y[0:ROWS, cols] + (direct - extra)
        gate[0:ROWS, cols] = short(qf, 0, 0, ROWS, cols)
        return 0

    lax.fori_loop(0, strips, patch, 0)
    column = min(256, width)

    def fetch(j):
        count = len(turns[j]) - (j == 0)
        arrive(starts_in.at[pl.ds(0, count)], s["down_recv"].at[j])

    def finish(strips_now, slot):
        for i, strip in enumerate(strips_now):
            cols = lanes(strip)
            terms = [gain[strip, m] * starts_in[strip, pl.ds(m, 1), :] for m in range(modes)]
            fades = [jnp.broadcast_to(drop[strip, pl.ds(m, 1), :], (ROWS, LANES)) for m in range(modes)]
            for block in range(0, blocks, 2):
                results = []
                for b in (block, block + 1):
                    result = y[pl.ds(b * ROWS, ROWS), cols]
                    for m in range(modes):
                        result = result + terms[m]
                    if b < blocks - 1:
                        terms = [term * fade for term, fade in zip(terms, fades, strict=True)]
                    results.append(gate[pl.ds(b * ROWS, ROWS), cols] * result.astype(bf16).astype(f32))
                both = jnp.concatenate(results, axis=0).astype(bf16)
                gated[slot, block * ROWS : (block + 2) * ROWS, i * LANES : (i + 1) * LANES] = both

    def project(strips_now, slot, begins, stops):
        size = len(strips_now) * LANES
        rows = pl.ds(pl.multiple_of(strips_now[0] * LANES, size), size)
        for n in range(width // column):
            cols = slice(n * column, (n + 1) * column)
            part = jnp.dot(gated[slot, :, 0:size], w_in[rows, cols], preferred_element_type=f32)
            if not begins:
                part = part + total[:, cols]
            if stops:
                out_ref[:, cols] = part.astype(out_ref.dtype)
            else:
                total[:, cols] = part

    turns = []
    for dy in reach:
        first = lax.rem(spot_y + dy, wide) * wide
        if dy == reach[-1]:
            for dx in range(0, wide, pair):
                at = first + lax.rem(spot_x // pair * pair + dx, wide)
                turns.append([at + i for i in range(pair)])
        else:
            turns.append([first + i for i in range(wide)])
    count = len(turns)
    fetch(0)
    finish(turns[0], 0)
    w_load.wait()
    for j in range(1, count):
        fetch(j)
        project(turns[j - 1], (j - 1) % 2, j == 1, False)
        finish(turns[j], j % 2)
    project(turns[count - 1], (count - 1) % 2, count == 1, True)
    @pl.when((spot < members - 1) | closing)
    def _():
        arrive(tails, s["halo_send"])

    arrive(edges.at[others], s["edge_send"])
    arrive(ends.at[others], s["up_send"])
    arrive(starts.at[others], s["down_send"])

    for i in range(1, planes):

        @pl.when(plane < i)
        def _():
            arrive(sums, s["side_send"].at[i - 1])


def body(planes, queries, keys, values, short_taps, decay, residue, skip, w_out):
    toks, width = queries.shape
    modes = decay.shape[1]
    held = scratch(planes, toks, width, modes)
    outside = pl.BlockSpec(memory_space=pltpu.HBM)
    return pl.pallas_call(
        functools.partial(kernel, planes, tuple(held)),
        out_shape=jax.ShapeDtypeStruct((toks, width), jnp.bfloat16),
        in_specs=[outside] * 8,
        out_specs=pl.BlockSpec(memory_space=pltpu.VMEM),
        scratch_shapes=list(held.values()),
        compiler_params=pltpu.CompilerParams(
            collective_id=0, has_side_effects=True, vmem_limit_bytes=48 * 1024 * 1024
        ),
    )(
        *(
            pltpu.with_memory_space_constraint(value, pltpu.HBM)
            for value in (
                queries, keys, values, short_taps, decay.T, residue.T,
                skip.reshape(width // LANES, LANES), w_out,
            )
        )
    )


def solution(mesh):
    split = P(("rep", "seq"), None)
    placed = (split, split, split, P(), P(), P(), P(), P())

    def run(queries, *rest):
        planes = mesh.shape["seq"] * LANES // queries.shape[1]
        return body(planes, queries, *rest)

    return jax.shard_map(run, mesh=mesh, in_specs=placed, out_specs=split, check_vma=False)
```
